32 devices in a mesh: data: 1 (over z), expert: 32 (over y, x, core).
Axes of the slice: x: 4, y: 4, z: 1, core: 2. Of those that a mesh axis runs over, the one named last changes fastest.
The devices are a block of a 4x4x8 slice.
Arguments:
- x_a: bfloat16 [32768, 768], P(('data', 'expert'))
- idx_a: int32 [32768, 1], P(('data', 'expert'))
- gate_a: float32 [32768, 1], P(('data', 'expert'))
- x_b: bfloat16 [32768, 768], P(('data', 'expert'))
- idx_b: int32 [32768, 1], P(('data', 'expert'))
- gate_b: float32 [32768, 1], P(('data', 'expert'))
- w_up: bfloat16 [128, 768, 3072], P('expert')
- w_down: bfloat16 [128, 3072, 768], P('expert')
Outputs:
- output 1: bfloat16 [32768, 768], P(('data', 'expert'))
- output 2: bfloat16 [32768, 768], P(('data', 'expert'))
All inputs are finite; a program needn't handle non-finite values.
Results may differ from the reference program's by a relative error of at most 0.001.
Values are sent between devices in bfloat16 or wider.
A program may use at most 768 MiB of HBM per device.

```python
import jax
import jax.numpy as jnp
from jax import lax

TOKENS_DEV = 1024
GROUP_SIZE = 32
MODEL_DIM = 768
FFN_DIM = 3072
EXPERTS = 128
TOP_K = 1
CAPACITY = 256


def draw_routing(rng_key):
    mean_load = TOKENS_DEV * TOP_K // EXPERTS
    half_count = EXPERTS // 2
    key_perm, key_devs = jax.random.split(rng_key)
    relabel = jax.random.permutation(key_perm, EXPERTS)
    dev_keys = jax.random.split(key_devs, GROUP_SIZE)

    def one_device(dev_key):
        sub_keys = jax.random.split(dev_key, 5)
        pair_shift = jax.random.randint(sub_keys[0], (half_count,), 0, mean_load + 1)
        full_pair = jax.random.randint(sub_keys[1], (), 0, half_count)
        pair_shift = jnp.where(jnp.arange(half_count) == full_pair, mean_load, pair_shift)
        pair_flip = jnp.where(jax.random.randint(sub_keys[2], (half_count,), 0, 4) < 3, 1, -1)
        pair_counts = jnp.stack([mean_load + pair_flip * pair_shift, mean_load - pair_flip * pair_shift], axis=1).reshape(EXPERTS)
        dev_counts = jnp.zeros((EXPERTS,), jnp.int32).at[relabel].set(pair_counts)
        range_ends = jnp.cumsum(dev_counts)
        sorted_ids = jnp.searchsorted(range_ends, jnp.arange(TOKENS_DEV * TOP_K), side='right')
        choice_tab = sorted_ids.reshape(TOP_K, TOKENS_DEV).T
        choice_tab = choice_tab[jax.random.permutation(sub_keys[3], TOKENS_DEV)]
        rot_rows = jax.random.randint(sub_keys[4], (TOKENS_DEV, 1), 0, TOP_K)
        col_ids = (jnp.arange(TOP_K)[None, :] + rot_rows) % TOP_K
        return jnp.take_along_axis(choice_tab, col_ids, axis=1).astype(jnp.int32)

    return jax.vmap(one_device)(dev_keys).reshape(GROUP_SIZE * TOKENS_DEV, TOP_K)


def setup_inputs(seed: int = 0, part: int = 0) -> dict:
    part_keys = jax.random.split(jax.random.fold_in(jax.random.key(seed), part), 6)
    weight_keys = jax.random.split(jax.random.key(seed + 1), 2)
    n_rows = GROUP_SIZE * TOKENS_DEV
    gate_scale = TOP_K ** -0.5
    x_a = jax.random.normal(part_keys[0], (n_rows, MODEL_DIM), jnp.float32).astype(jnp.bfloat16)
    idx_a = draw_routing(part_keys[1])
    gate_a = jax.random.uniform(part_keys[2], (n_rows, TOP_K), jnp.float32, 0.5, 1.5) * gate_scale
    x_b = jax.random.normal(part_keys[3], (n_rows, MODEL_DIM), jnp.float32).astype(jnp.bfloat16)
    idx_b = draw_routing(part_keys[4])
    gate_b = jax.random.uniform(part_keys[5], (n_rows, TOP_K), jnp.float32, 0.5, 1.5) * gate_scale
    w_up = (jax.random.normal(weight_keys[0], (EXPERTS, MODEL_DIM, FFN_DIM), jnp.float32) * MODEL_DIM ** -0.5).astype(jnp.bfloat16)
    w_down = (jax.random.normal(weight_keys[1], (EXPERTS, FFN_DIM, MODEL_DIM), jnp.float32) * FFN_DIM ** -0.5).astype(jnp.bfloat16)
    return dict(x_a=x_a, idx_a=idx_a, gate_a=gate_a, x_b=x_b, idx_b=idx_b, gate_b=gate_b, w_up=w_up, w_down=w_down)


def moe_layer(tok_rows, route_ids, gate_vals, w_up, w_down):
    n_rows = GROUP_SIZE * TOKENS_DEV
    n_pairs = n_rows * TOP_K
    flat_ids = route_ids.reshape(n_pairs)
    sort_order = jnp.argsort(flat_ids, stable=True)
    counts = jnp.zeros((EXPERTS,), jnp.int32).at[flat_ids].add(1)
    starts = jnp.cumsum(counts) - counts
    sorted_rank = jnp.arange(n_pairs, dtype=jnp.int32) - starts[flat_ids[sort_order]]
    slot_rank = jnp.zeros((n_pairs,), jnp.int32).at[sort_order].set(sorted_rank)
    slot_index = jnp.where(slot_rank < CAPACITY, flat_ids * CAPACITY + slot_rank, EXPERTS * CAPACITY)
    pair_token = jnp.arange(n_pairs, dtype=jnp.int32) // TOP_K
    buffer = jnp.zeros((EXPERTS * CAPACITY, MODEL_DIM), jnp.bfloat16).at[slot_index].set(tok_rows[pair_token], mode='drop')

    def expert_ffn(operands):
        rows_in, up_mat, down_mat = operands
        hidden = jax.nn.gelu(jnp.dot(rows_in, up_mat, preferred_element_type=jnp.float32)).astype(jnp.bfloat16)
        return jnp.dot(hidden, down_mat, preferred_element_type=jnp.float32).astype(jnp.bfloat16)

    expert_out = lax.map(expert_ffn, (buffer.reshape(EXPERTS, CAPACITY, MODEL_DIM), w_up, w_down))
    pair_out = jnp.take(expert_out.reshape(EXPERTS * CAPACITY, MODEL_DIM), slot_index, axis=0, mode='fill', fill_value=0)
    pair_out = pair_out.astype(jnp.float32).reshape(n_rows, TOP_K, MODEL_DIM)
    mix_sum = jnp.sum(gate_vals[:, :, None] * pair_out, axis=1)
    return (tok_rows.astype(jnp.float32) + mix_sum).astype(jnp.bfloat16)


def reference(x_a, idx_a, gate_a, x_b, idx_b, gate_b, w_up, w_down):
    y_a = moe_layer(x_a, idx_a, gate_a, w_up, w_down)
    y_b = moe_layer(x_b, idx_b, gate_b, w_up, w_down)
    return (y_a, y_b)
```

```python
import functools

import jax
import jax.numpy as jnp
from jax import lax
from jax.experimental import pallas as pl
from jax.experimental.pallas import tpu as pltpu
from jax.sharding import PartitionSpec as P

BF16 = jnp.bfloat16
F32 = jnp.float32
LANES = 128


def iota(shape, dim):
    return lax.broadcasted_iota(jnp.int32, shape, dim)


def one_hot(mask):
    return jnp.where(mask, 1.0, 0.0).astype(BF16)


def dot(a, b):
    return jnp.dot(a, b, preferred_element_type=F32)


def dot_nt(a, b):
    return lax.dot_general(a, b, (((1,), (1,)), ((), ())), preferred_element_type=F32)


def to_column(row):
    return jnp.transpose(jnp.broadcast_to(row, (LANES, row.shape[1])))


def lane_match(column, width, base):
    lane = iota(column.shape, 1)
    parts = [one_hot(column == lane + (base + k * LANES)) for k in range(width // LANES)]
    return jnp.concatenate(parts, axis=1)


def kernel(group, stride, ids_a, gate_a, ids_b, gate_b, x_a, x_b, w_up, w_down, y_a, y_b,
           x_v, send, recv, back, counts, table, w1, w2, hidden, rows_in, acc, y_v,
           posc, slotr, slotc,
           x_sem, y_sem, w_sem, count_sems, send_sems, recv_sems, ret_sems, back_sems):
    me = lax.axis_index('expert')
    local, _, load, dim = send.shape[1:]
    n_tok = x_v.shape[1]
    n_exp = local * group
    span = group * load
    cap = rows_in.shape[0]
    ffn = hidden.shape[1]
    ids_refs, gate_refs = (ids_a, ids_b), (gate_a, gate_b)
    x_refs, y_refs = (x_a, x_b), (y_a, y_b)

    def peer(i):
        return lax.rem(me + i * stride, group)

    barrier = pltpu.get_barrier_semaphore()

    @pl.loop(1, group)
    def _(i):
        pl.semaphore_signal(barrier, inc=1, device_id={'expert': peer(i)}, device_id_type=pl.DeviceIdType.MESH)

    def x_copy(m):
        return pltpu.make_async_copy(x_refs[m], x_v.at[m], x_sem.at[m])

    def y_copy(m):
        return pltpu.make_async_copy(y_v.at[m], y_refs[m], y_sem.at[m])

    def w_copies(e, slot):
        return (pltpu.make_async_copy(w_up.at[e], w1.at[slot], w_sem.at[slot, 0]),
                pltpu.make_async_copy(w_down.at[e], w2.at[slot], w_sem.at[slot, 1]))

    x_copy(0).start()
    x_copy(1).start()
    for e in range(2):
        for copy in w_copies(e, e):
            copy.start()

    upper = one_hot(iota((n_tok, n_tok), 0) < iota((n_tok, n_tok), 1))
    pos_rows, count_rows = [], []
    for m in range(2):
        ids = ids_refs[m][...]
        hot = one_hot(iota((n_exp, n_tok), 0) == ids)
        earlier = dot(hot, upper)
        rank = jnp.sum(hot.astype(F32) * earlier, axis=0, keepdims=True).astype(jnp.int32)
        count_rows.append(dot_nt(jnp.ones((8, n_tok), BF16), hot))
        pos = lax.rem(ids, local) * span + lax.div(ids, local) * load + rank
        pos_rows.append(pos)
        posc[m] = to_column(pos)
    counts[...] = jnp.where(iota((8, n_exp), 0) < 4, count_rows[0], count_rows[1])

    def gather_rows(m):
        x_copy(m).wait()

        @pl.loop(0, local)
        def _(e):
            pick = one_hot(iota((span, n_tok), 0) == pos_rows[m] - e * span)
            send[m, e] = dot(pick, x_v[m]).astype(BF16).reshape(group, load, dim)

    def dispatch(m):
        pltpu.make_async_copy(send.at[m, :, me], recv.at[m, :, me], recv_sems.at[m]).start()

        @pl.loop(1, group)
        def _(i):
            pltpu.make_async_remote_copy(
                src_ref=send.at[m, :, peer(i)], dst_ref=recv.at[m, :, me],
                send_sem=send_sems.at[m], recv_sem=recv_sems.at[m],
                device_id={'expert': peer(i)}, device_id_type=pl.DeviceIdType.MESH).start()

    def give_back(m, e):
        pltpu.make_async_copy(recv.at[m, e, me], back.at[m, e, me], back_sems.at[m, e]).start()

        @pl.loop(1, group)
        def _(i):
            pltpu.make_async_remote_copy(
                src_ref=recv.at[m, e, peer(i)], dst_ref=back.at[m, e, me],
                send_sem=ret_sems.at[m], recv_sem=back_sems.at[m, e],
                device_id={'expert': peer(i)}, device_id_type=pl.DeviceIdType.MESH).start()

    gather_rows(0)
    pl.semaphore_wait(barrier, group - 1)

    pltpu.make_async_copy(counts, table.at[me], count_sems.at[1]).start()

    @pl.loop(1, group)
    def _(i):
        pltpu.make_async_remote_copy(
            src_ref=counts, dst_ref=table.at[me],
            send_sem=count_sems.at[0], recv_sem=count_sems.at[1],
            device_id={'expert': peer(i)}, device_id_type=pl.DeviceIdType.MESH).start()

    dispatch(0)
    gather_rows(1)
    dispatch(1)

    pltpu.make_async_copy(table, table, count_sems.at[1]).wait()
    lower = one_hot(iota((group, group), 1) <= iota((group, group), 0))
    mine = one_hot(iota((8, n_exp), 1) - me * local == iota((8, n_exp), 0))
    mine = jnp.where(iota((8, n_exp), 0) < local, mine.astype(F32), 0.0).astype(BF16)
    spread = one_hot(lax.div(iota((group, span), 1), load) == iota((group, span), 0))
    row_in_load = lax.rem(iota((8, span), 1), load)
    for m in range(2):
        cnt = table[:, 4 * m, :]
        inclusive = dot(lower, cnt.astype(BF16))
        first = jnp.minimum(inclusive - cnt, float(cap))
        kept = jnp.minimum(inclusive, float(cap)) - first
        first_row = dot(dot_nt(mine, first.astype(BF16)).astype(BF16), spread).astype(jnp.int32)
        kept_row = dot(dot_nt(mine, kept.astype(BF16)).astype(BF16), spread).astype(jnp.int32)
        slot = jnp.where(row_in_load < kept_row, first_row + row_in_load, -1)
        for e in range(local):
            row = slot[e:e + 1]
            slotr[m, e] = jnp.broadcast_to(row, (8, span))
            slotc[m, e] = to_column(row)

    tile = min(512, ffn)

    def experts(m):
        pltpu.make_async_copy(recv.at[m], recv.at[m], recv_sems.at[m]).wait()

        @pl.loop(0, local)
        def _(e):
            step = m * local + e
            slot = lax.rem(step, 2)
            pick = one_hot(iota((cap, span), 0) == slotr[m, e, 0:1])
            rows_in[...] = dot(pick, recv[m, e].reshape(span, dim)).astype(BF16)
            for copy in w_copies(e, slot):
                copy.wait()

            @pl.loop(0, ffn // tile)
            def _(f):
                cols = pl.ds(pl.multiple_of(f * tile, tile), tile)
                hidden[:, cols] = jax.nn.gelu(dot(rows_in[...], w1[slot, :, cols])).astype(BF16)

            out = dot(hidden[...], w2[slot]).astype(BF16)
            place = lane_match(slotc[m, e], cap, 0)
            recv[m, e] = dot(place, out).astype(BF16).reshape(group, load, dim)
            give_back(m, e)

            @pl.when(step + 2 < 2 * local)
            def _():
                for copy in w_copies(lax.rem(e + 2, local), slot):
                    copy.start()

    experts(0)
    experts(1)

    rows = min(256, n_tok)

    def combine(m):
        for e in range(local):
            pltpu.make_async_copy(back.at[m, e], back.at[m, e], back_sems.at[m, e]).wait()

            @pl.loop(0, n_tok // rows)
            def _(b):
                part = pl.ds(pl.multiple_of(b * rows, rows), rows)
                take = lane_match(posc[m, part], span, e * span)
                got = dot(take, back[m, e].reshape(span, dim))
                if e > 0:
                    got = got + acc[part]
                acc[part] = got

        gate_col = to_column(gate_refs[m][...])
        for k in range(dim // LANES):
            cols = slice(k * LANES, (k + 1) * LANES)
            y_v[m, :, cols] = (x_v[m, :, cols].astype(F32) + gate_col * acc[:, cols]).astype(BF16)
        y_copy(m).start()

    combine(0)
    combine(1)

    pltpu.make_async_copy(table.at[0:group - 1], table.at[0:group - 1], count_sems.at[0]).wait()
    for m in range(2):
        sent = send.at[m, :, 0:group - 1]
        pltpu.make_async_copy(sent, sent, send_sems.at[m]).wait()
        pltpu.make_async_copy(sent, sent, ret_sems.at[m]).wait()
        y_copy(m).wait()


def moe(group, x_a, idx_a, gate_a, x_b, idx_b, gate_b, w_up, w_down):
    n_tok, dim = x_a.shape
    local, _, ffn = w_up.shape
    n_exp = local * group
    load = 2 * n_tok // n_exp
    cap = n_tok // local
    span = group * load
    rows = [a.reshape(1, n_tok) for a in (idx_a, gate_a, idx_b, gate_b)]
    vmem, hbm = pl.BlockSpec(memory_space=pltpu.VMEM), pl.BlockSpec(memory_space=pl.ANY)
    dma = pltpu.SemaphoreType.DMA
    exchange = (2, local, group, load, dim)
    return pl.pallas_call(
        functools.partial(kernel, group, 11),
        out_shape=(jax.ShapeDtypeStruct((n_tok, dim), BF16),) * 2,
        in_specs=[vmem] * 4 + [hbm] * 4,
        out_specs=(hbm, hbm),
        scratch_shapes=[
            pltpu.VMEM((2, n_tok, dim), BF16),
            pltpu.VMEM(exchange, BF16),
            pltpu.VMEM(exchange, BF16),
            pltpu.VMEM(exchange, BF16),
            pltpu.VMEM((8, n_exp), F32),
            pltpu.VMEM((group, 8, n_exp), F32),
            pltpu.VMEM((2, dim, ffn), BF16),
            pltpu.VMEM((2, ffn, dim), BF16),
            pltpu.VMEM((cap, ffn), BF16),
            pltpu.VMEM((cap, dim), BF16),
            pltpu.VMEM((n_tok, dim), F32),
            pltpu.VMEM((2, n_tok, dim), BF16),
            pltpu.VMEM((2, n_tok, LANES), jnp.int32),
            pltpu.VMEM((2, local, 8, span), jnp.int32),
            pltpu.VMEM((2, local, span, LANES), jnp.int32),
            dma((2,)), dma((2,)), dma((2, 2)), dma((2,)), dma((2,)), dma((2,)), dma((2,)), dma((2, local)),
        ],
        compiler_params=pltpu.CompilerParams(
            collective_id=0, has_side_effects=True, vmem_limit_bytes=64 * 1024 * 1024 - 65536),
        name='moe',
    )(*rows, x_a, x_b, w_up, w_down)


def solution(mesh):
    row_spec = P(('data', 'expert'), None)
    weight_spec = P('expert', None, None)
    return jax.shard_map(
        functools.partial(moe, mesh.shape['expert']), mesh=mesh,
        in_specs=(row_spec,) * 6 + (weight_spec,) * 2, out_specs=(row_spec, row_spec), check_vma=False)
```

```python
import functools
import math

import jax
import jax.numpy as jnp
from jax import lax
from jax.experimental import pallas as pl
from jax.experimental.pallas import tpu as pltpu
from jax.sharding import PartitionSpec as P

BF16 = jnp.bfloat16
F32 = jnp.float32
LANES = 128


def iota(shape, dim):
    return lax.broadcasted_iota(jnp.int32, shape, dim)


def one_hot(mask):
    return jnp.where(mask, 1.0, 0.0).astype(BF16)


def dot(a, b):
    return jnp.dot(a, b, preferred_element_type=F32)


def dot_nt(a, b):
    return lax.dot_general(a, b, (((1,), (1,)), ((), ())), preferred_element_type=F32)


def to_column(row):
    return jnp.transpose(jnp.broadcast_to(row, (LANES, row.shape[1])))


def lane_match(column, width, base):
    lane = iota(column.shape, 1)
    parts = [one_hot(column == lane + (base + k * LANES)) for k in range(width // LANES)]
    return jnp.concatenate(parts, axis=1)


def displacements(side):
    turns = list(range(1, side)) + [0]
    back = [(side - d) % side for d in turns]
    ahead = range(1, (side + 1) // 2)
    queues = [[(dx, d) for dx in ahead for d in turns],
              [(side - dx, d) for dx in ahead for d in back],
              [(side // 2, d) for d in turns] if side % 2 == 0 else [],
              [(0, d) for d in turns if d]]
    steps = max(len(q) for q in queues)
    order = [q[i] for i in range(steps) for q in queues if i < len(q)]
    return [(dx, dy, flip) for dx, dy in order for flip in (0, 1)] + [(0, 0, 1)]


def kernel(group, ids_a, gate_a, ids_b, gate_b, x_a, x_b, w_up, w_down, y_a, y_b,
           x_v, send, recv, back, counts, table, w1, w2, hidden, rows_in, acc, y_v,
           posc, gatec, slotr, slotc, takes,
           x_sem, y_sem, w_sem, count_sems, send_sems, recv_sems, ret_sems, back_sems):
    me = lax.axis_index('expert')
    local, _, load, dim = send.shape[1:]
    n_tok = x_v.shape[1]
    n_exp = local * group
    span = group * load
    cap = rows_in.shape[0]
    ffn = hidden.shape[1]
    ids_refs, gate_refs = (ids_a, ids_b), (gate_a, gate_b)
    x_refs, y_refs = (x_a, x_b), (y_a, y_b)

    side = math.isqrt(group // 2)
    core = lax.rem(me, 2)
    my_x, my_y = lax.rem(lax.div(me, 2), side), lax.div(me, 2 * side)
    hops = displacements(side)

    def towards(dx, dy, flip):
        x = lax.rem(my_x + dx + core * (side - 2 * dx), side)
        y = lax.rem(my_y + dy + core * (side - 2 * dy), side)
        return (y * side + x) * 2 + lax.rem(core + flip, 2)

    def peer(i):
        return lax.rem(me + i, group)

    barrier = pltpu.get_barrier_semaphore()

    @pl.loop(1, group)
    def _(i):
        pl.semaphore_signal(barrier, inc=1, device_id={'expert': peer(i)}, device_id_type=pl.DeviceIdType.MESH)

    def x_copy(m):
        return pltpu.make_async_copy(x_refs[m], x_v.at[m], x_sem.at[m])

    def w_copies(e, slot):
        return (pltpu.make_async_copy(w_up.at[e], w1.at[slot], w_sem.at[slot, 0]),
                pltpu.make_async_copy(w_down.at[e], w2.at[slot], w_sem.at[slot, 1]))

    x_copy(0).start()
    x_copy(1).start()
    for e in range(2):
        for copy in w_copies(e, e):
            copy.start()

    before = one_hot(iota((LANES, LANES), 0) < iota((LANES, LANES), 1))
    ones = jnp.ones((8, n_tok), BF16)

    def positions(m):
        ids = ids_refs[m][...]
        hot = one_hot(iota((n_exp, n_tok), 0) == ids)
        seen = jnp.zeros((n_exp, 1), F32)
        ranks = []
        for k in range(n_tok // LANES):
            block = hot[:, k * LANES:(k + 1) * LANES]
            wide = block.astype(F32)
            ranks.append(jnp.sum(wide * (dot(block, before) + seen), axis=0, keepdims=True))
            seen = seen + jnp.sum(wide, axis=1, keepdims=True)
        rank = jnp.concatenate(ranks, axis=1).astype(jnp.int32)
        pos = lax.rem(ids, local) * span + lax.div(ids, local) * load + rank
        return pos, hot

    def gather_rows(m, pos):
        x_copy(m).wait()

        @pl.loop(0, local)
        def _(e):
            pick = one_hot(iota((span, n_tok), 0) == pos - e * span)
            send[m, e] = dot(pick, x_v[m]).astype(BF16).reshape(group, load, dim)

    def push(src, dst, send_sem, recv_sem, to):
        pltpu.make_async_remote_copy(
            src_ref=src, dst_ref=dst, send_sem=send_sem, recv_sem=recv_sem,
            device_id={'expert': to}, device_id_type=pl.DeviceIdType.MESH).start()

    def dispatch(m, part):
        pltpu.make_async_copy(send.at[m, part, me], recv.at[m, part, me], recv_sems.at[m]).start()
        for hop in hops:
            to = towards(*hop)
            push(send.at[m, part, to], recv.at[m, part, me], send_sems.at[m], recv_sems.at[m], to)

    def give_back(m, e):
        pltpu.make_async_copy(recv.at[m, e, me], back.at[m, e, me], back_sems.at[m, e]).start()
        for hop in hops:
            to = towards(*hop)
            push(recv.at[m, e, to], back.at[m, e, me], ret_sems.at[m], back_sems.at[m, e], to)

    half = local // 2
    pos_a, hot_a = positions(0)
    gather_rows(0, pos_a)
    pl.semaphore_wait(barrier, group - 1)
    dispatch(0, slice(0, local))
    pos_b, hot_b = positions(1)
    gather_rows(1, pos_b)
    dispatch(1, slice(0, half))

    counts[...] = jnp.where(iota((8, n_exp), 0) < 4, dot_nt(ones, hot_a), dot_nt(ones, hot_b))
    for m, pos in enumerate((pos_a, pos_b)):
        posc[m] = to_column(pos)
        gatec[m] = to_column(gate_refs[m][...])
    pltpu.make_async_copy(counts, table.at[me], count_sems.at[1]).start()

    @pl.loop(1, group)
    def _(i):
        push(counts, table.at[me], count_sems.at[0], count_sems.at[1], peer(i))

    pltpu.make_async_copy(table, table, count_sems.at[1]).wait()
    lower = one_hot(iota((group, group), 1) <= iota((group, group), 0))
    mine = one_hot(iota((8, n_exp), 1) - me * local == iota((8, n_exp), 0))
    mine = jnp.where(iota((8, n_exp), 0) < local, mine.astype(F32), 0.0).astype(BF16)
    spread = one_hot(lax.div(iota((group, span), 1), load) == iota((group, span), 0))
    row_in_load = lax.rem(iota((8, span), 1), load)
    for m in range(2):
        cnt = table[:, 4 * m, :]
        inclusive = dot(lower, cnt.astype(BF16))
        first = jnp.minimum(inclusive - cnt, float(cap))
        kept = jnp.minimum(inclusive, float(cap)) - first
        first_row = dot(dot_nt(mine, first.astype(BF16)).astype(BF16), spread).astype(jnp.int32)
        kept_row = dot(dot_nt(mine, kept.astype(BF16)).astype(BF16), spread).astype(jnp.int32)
        slot = jnp.where(row_in_load < kept_row, first_row + row_in_load, -1)
        for e in range(local):
            row = slot[e:e + 1]
            slotr[m, e] = jnp.broadcast_to(row, (8, span))
            slotc[m, e] = to_column(row)

    tile = min(512, ffn)

    def experts(m):
        pltpu.make_async_copy(recv.at[m], recv.at[m], recv_sems.at[m]).wait()
        if m == 0:
            dispatch(1, slice(half, local))

        @pl.loop(0, local)
        def _(e):
            step = m * local + e
            slot = lax.rem(step, 2)
            pick = one_hot(iota((cap, span), 0) == slotr[m, e, 0:1])
            rows_in[...] = dot(pick, recv[m, e].reshape(span, dim)).astype(BF16)
            for copy in w_copies(e, slot):
                copy.wait()

            @pl.loop(0, ffn // tile)
            def _(f):
                cols = pl.ds(pl.multiple_of(f * tile, tile), tile)
                hidden[:, cols] = jax.nn.gelu(dot(rows_in[...], w1[slot, :, cols])).astype(BF16)

            out = dot(hidden[...], w2[slot]).astype(BF16)
            place = lane_match(slotc[m, e], cap, 0)
            recv[m, e] = dot(place, out).astype(BF16).reshape(group, load, dim)
            give_back(m, e)

            @pl.when(step + 2 < 2 * local)
            def _():
                for copy in w_copies(lax.rem(e + 2, local), slot):
                    copy.start()

    experts(0)
    experts(1)

    rows = min(256, n_tok)
    last = local - 1

    def combine(m):
        @pl.loop(0, n_tok // rows)
        def _(b):
            part = pl.ds(pl.multiple_of(b * rows, rows), rows)
            takes[part] = lane_match(posc[m, part], span, last * span)

        for e in range(local):
            pltpu.make_async_copy(back.at[m, e], back.at[m, e], back_sems.at[m, e]).wait()

            @pl.loop(0, n_tok // rows)
            def _(b):
                part = pl.ds(pl.multiple_of(b * rows, rows), rows)
                take = takes[part] if e == last else lane_match(posc[m, part], span, e * span)
                got = dot(take, back[m, e].reshape(span, dim))
                if e > 0:
                    got = got + acc[part]
                if e < last:
                    acc[part] = got
                else:
                    gate = jnp.concatenate([gatec[m, part]] * (dim // LANES), axis=1)
                    y_v[m, part] = (x_v[m, part].astype(F32) + gate * got).astype(BF16)
                    pltpu.make_async_copy(y_v.at[m, part], y_refs[m].at[part], y_sem.at[m]).start()

    combine(0)
    combine(1)

    pltpu.make_async_copy(table.at[0:group - 1], table.at[0:group - 1], count_sems.at[0]).wait()
    for m in range(2):
        sent = send.at[m, :, 0:group - 1]
        pltpu.make_async_copy(sent, sent, send_sems.at[m]).wait()
        pltpu.make_async_copy(sent, sent, ret_sems.at[m]).wait()
        pltpu.make_async_copy(y_v.at[m], y_refs[m], y_sem.at[m]).wait()


def moe(group, x_a, idx_a, gate_a, x_b, idx_b, gate_b, w_up, w_down):
    n_tok, dim = x_a.shape
    local, _, ffn = w_up.shape
    n_exp = local * group
    load = 2 * n_tok // n_exp
    cap = n_tok // local
    span = group * load
    rows = [a.reshape(1, n_tok) for a in (idx_a, gate_a, idx_b, gate_b)]
    vmem, hbm = pl.BlockSpec(memory_space=pltpu.VMEM), pl.BlockSpec(memory_space=pl.ANY)
    dma = pltpu.SemaphoreType.DMA
    exchange = (2, local, group, load, dim)
    return pl.pallas_call(
        functools.partial(kernel, group),
        out_shape=(jax.ShapeDtypeStruct((n_tok, dim), BF16),) * 2,
        in_specs=[vmem] * 4 + [hbm] * 4,
        out_specs=(hbm, hbm),
        scratch_shapes=[
            pltpu.VMEM((2, n_tok, dim), BF16),
            pltpu.VMEM(exchange, BF16),
            pltpu.VMEM(exchange, BF16),
            pltpu.VMEM(exchange, BF16),
            pltpu.VMEM((8, n_exp), F32),
            pltpu.VMEM((group, 8, n_exp), F32),
            pltpu.VMEM((2, dim, ffn), BF16),
            pltpu.VMEM((2, ffn, dim), BF16),
            pltpu.VMEM((cap, ffn), BF16),
            pltpu.VMEM((cap, dim), BF16),
            pltpu.VMEM((n_tok, dim), F32),
            pltpu.VMEM((2, n_tok, dim), BF16),
            pltpu.VMEM((2, n_tok, LANES), jnp.int32),
            pltpu.VMEM((2, n_tok, LANES), F32),
            pltpu.VMEM((2, local, 8, span), jnp.int32),
            pltpu.VMEM((2, local, span, LANES), jnp.int32),
            pltpu.VMEM((n_tok, span), BF16),
            dma((2,)), dma((2,)), dma((2, 2)), dma((2,)), dma((2,)), dma((2,)), dma((2,)), dma((2, local)),
        ],
        compiler_params=pltpu.CompilerParams(
            collective_id=0, has_side_effects=True, vmem_limit_bytes=64 * 1024 * 1024 - 65536),
        name='moe',
    )(*rows, x_a, x_b, w_up, w_down)


def solution(mesh):
    row_spec = P(('data', 'expert'), None)
    weight_spec = P('expert', None, None)
    return jax.shard_map(
        functools.partial(moe, mesh.shape['expert']), mesh=mesh,
        in_specs=(row_spec,) * 6 + (weight_spec,) * 2, out_specs=(row_spec, row_spec), check_vma=False)
```
